16 devices in a mesh: dp: 2 (over z), ep: 8 (over y, x, core).
Axes of the slice: x: 2, y: 2, z: 2, core: 2. Of those that a mesh axis runs over, the one named last changes fastest.
Arguments:
- tok_x: bfloat16 [16384, 4096], P(('dp', 'ep'))
- tok_dy: bfloat16 [16384, 4096], P(('dp', 'ep'))
- exp_first: int32 [16384], P(('dp', 'ep'))
- exp_second: int32 [16384], P(('dp', 'ep'))
- eligible: int32 [16384, 8], P(('dp', 'ep'))
- slot_first: int32 [16384], P(('dp', 'ep'))
- slot_second: int32 [16384], P(('dp', 'ep'))
- ln_weight: bfloat16 [4096], replicated
- ln_bias: bfloat16 [4096], replicated
- router: bfloat16 [4096, 8], replicated
- w_gate: bfloat16 [8, 4096, 1376], P('ep')
- w_up: bfloat16 [8, 4096, 1376], P('ep')
- w_down: bfloat16 [8, 1376, 4096], P('ep')
Outputs:
- output 1: bfloat16 [16384, 4096], P(('dp', 'ep'))
- output 2: bfloat16 [16384, 4096], P(('dp', 'ep'))
- output 3: float32 [8, 4096, 1376], P('ep')
- output 4: float32 [8, 4096, 1376], P('ep')
- output 5: float32 [8, 1376, 4096], P('ep')
- output 6: float32 [4096, 8], replicated
- output 7: float32 [4096], replicated
- output 8: float32 [4096], replicated
All inputs are finite; a program needn't handle non-finite values.
Results may differ from the reference program's by a relative error of at most 0.00493557.
Values are sent between devices in bfloat16 or wider.
A program may use at most 1 GiB of HBM per device.

```python
import jax
import jax.numpy as jnp
from jax import lax

SHARDS = 16
TOK_DEV = 1024
D_MODEL = 4096
FF_DIM = 1376
EXPERTS = 8
SLOT_CAP = 384
LN_EPS = 1e-5


def draw_routing(rng_key):
    n_tok = SHARDS * TOK_DEV
    key_list = jax.random.split(rng_key, 5)
    pick_a = jax.random.randint(key_list[0], (n_tok,), 0, EXPERTS)
    pick_b = jax.random.randint(key_list[1], (n_tok,), 0, EXPERTS)
    pick_c = jax.random.randint(key_list[2], (n_tok,), 0, EXPERTS)
    first_pick = jnp.minimum(jnp.minimum(pick_a, pick_b), pick_c)
    second_pick = (first_pick + 1 + jax.random.randint(key_list[3], (n_tok,), 0, EXPERTS - 1)) % EXPERTS
    expert_ids = jnp.arange(EXPERTS)
    hot_first = (first_pick[:, None] == expert_ids[None, :]).astype(jnp.int32)
    hot_second = (second_pick[:, None] == expert_ids[None, :]).astype(jnp.int32)
    extra_bits = (jax.random.randint(key_list[4], (n_tok, EXPERTS), 0, 8) == 0).astype(jnp.int32)
    eligible = jnp.maximum(extra_bits, jnp.maximum(hot_first, hot_second))
    per_first = hot_first.reshape(SHARDS, TOK_DEV, EXPERTS)
    per_second = hot_second.reshape(SHARDS, TOK_DEV, EXPERTS)
    rank_first = jnp.sum((jnp.cumsum(per_first, axis=1) - per_first) * per_first, axis=2).reshape(n_tok)
    used_first = jnp.sum(per_first, axis=1, keepdims=True)
    rank_second = jnp.sum((jnp.cumsum(per_second, axis=1) - per_second + used_first) * per_second, axis=2).reshape(n_tok)
    slot_first = jnp.where(rank_first < SLOT_CAP, rank_first, -1)
    slot_second = jnp.where(rank_second < SLOT_CAP, rank_second, -1)
    return first_pick, second_pick, eligible, slot_first, slot_second


def setup_inputs(seed: int = 0) -> dict:
    key_list = jax.random.split(jax.random.key(seed), 10)
    n_tok = SHARDS * TOK_DEV
    first_pick, second_pick, eligible, slot_first, slot_second = draw_routing(key_list[0])
    tok_x = jax.random.normal(key_list[1], (n_tok, D_MODEL), jnp.float32).astype(jnp.bfloat16)
    tok_dy = jax.random.normal(key_list[2], (n_tok, D_MODEL), jnp.float32).astype(jnp.bfloat16)
    ln_weight = (1.0 + 0.3 * jax.random.normal(key_list[3], (D_MODEL,), jnp.float32)).astype(jnp.bfloat16)
    ln_bias = (0.3 * jax.random.normal(key_list[4], (D_MODEL,), jnp.float32)).astype(jnp.bfloat16)
    router = (1.5 * D_MODEL ** -0.5 * jax.random.normal(key_list[5], (D_MODEL, EXPERTS), jnp.float32)).astype(jnp.bfloat16)
    w_gate = (D_MODEL ** -0.5 * jax.random.normal(key_list[6], (EXPERTS, D_MODEL, FF_DIM), jnp.float32)).astype(jnp.bfloat16)
    w_up = (D_MODEL ** -0.5 * jax.random.normal(key_list[7], (EXPERTS, D_MODEL, FF_DIM), jnp.float32)).astype(jnp.bfloat16)
    w_down = (3.0 * FF_DIM ** -0.5 * jax.random.normal(key_list[8], (EXPERTS, FF_DIM, D_MODEL), jnp.float32)).astype(jnp.bfloat16)
    return {'tok_x': tok_x, 'tok_dy': tok_dy, 'exp_first': first_pick, 'exp_second': second_pick,
            'eligible': eligible, 'slot_first': slot_first, 'slot_second': slot_second,
            'ln_weight': ln_weight, 'ln_bias': ln_bias, 'router': router,
            'w_gate': w_gate, 'w_up': w_up, 'w_down': w_down}


def layer_norm(x_rows, ln_weight, ln_bias):
    x_float = x_rows.astype(jnp.float32)
    centered = x_float - jnp.mean(x_float, axis=-1, keepdims=True)
    inv_std = lax.rsqrt(jnp.mean(centered * centered, axis=-1, keepdims=True) + LN_EPS)
    x_hat = centered * inv_std
    hidden = (x_hat * ln_weight.astype(jnp.float32) + ln_bias.astype(jnp.float32)).astype(jnp.bfloat16)
    return hidden, x_hat, inv_std


def layer_norm_back(grad_h, x_hat, inv_std, ln_weight):
    scaled = grad_h * ln_weight.astype(jnp.float32)
    return inv_std * (scaled - jnp.mean(scaled, axis=-1, keepdims=True)
                      - x_hat * jnp.mean(scaled * x_hat, axis=-1, keepdims=True))


def masked_gate(logits, allowed, choice):
    expert_ids = jnp.arange(logits.shape[-1])
    prob_all = jax.nn.softmax(jnp.where(allowed, logits, -1e30), axis=-1)
    picked = (choice[:, None] == expert_ids[None, :]).astype(jnp.float32)
    return jnp.sum(prob_all * picked, axis=-1), prob_all, picked


def expert_pass(operands):
    hid_rows, grad_rows, gate_w, up_w, down_w = operands
    pre_gate = jnp.dot(hid_rows, gate_w, preferred_element_type=jnp.float32)
    pre_up = jnp.dot(hid_rows, up_w, preferred_element_type=jnp.float32)
    sig_gate = jax.nn.sigmoid(pre_gate)
    silu_gate = pre_gate * sig_gate
    inner_act = (silu_gate * pre_up).astype(jnp.bfloat16)
    exp_out = jnp.dot(inner_act, down_w, preferred_element_type=jnp.float32).astype(jnp.bfloat16)
    grad_inner = jnp.dot(grad_rows, down_w.T, preferred_element_type=jnp.float32)
    grad_pre_gate = (grad_inner * pre_up * sig_gate * (1.0 + pre_gate * (1.0 - sig_gate))).astype(jnp.bfloat16)
    grad_pre_up = (grad_inner * silu_gate).astype(jnp.bfloat16)
    grad_hid = (jnp.dot(grad_pre_gate, gate_w.T, preferred_element_type=jnp.float32)
                + jnp.dot(grad_pre_up, up_w.T, preferred_element_type=jnp.float32)).astype(jnp.bfloat16)
    dw_gate = jnp.dot(hid_rows.T, grad_pre_gate, preferred_element_type=jnp.float32)
    dw_up = jnp.dot(hid_rows.T, grad_pre_up, preferred_element_type=jnp.float32)
    dw_down = jnp.dot(inner_act.T, grad_rows, preferred_element_type=jnp.float32)
    return exp_out, grad_hid, dw_gate, dw_up, dw_down


def reference(tok_x, tok_dy, exp_first, exp_second, eligible, slot_first, slot_second,
              ln_weight, ln_bias, router, w_gate, w_up, w_down):
    n_tok = tok_x.shape[0]
    hidden, x_hat, inv_std = layer_norm(tok_x, ln_weight, ln_bias)
    logits = jnp.dot(hidden, router, preferred_element_type=jnp.float32)
    expert_ids = jnp.arange(EXPERTS)
    allowed = eligible > 0
    gate_one, prob_one, pick_one = masked_gate(logits, allowed, exp_first)
    gate_two, prob_two, pick_two = masked_gate(logits, allowed & (expert_ids[None, :] != exp_first[:, None]), exp_second)
    n_rows = EXPERTS * SHARDS * SLOT_CAP
    shard_idx = jnp.arange(n_tok) // TOK_DEV
    row_one = jnp.where(slot_first >= 0, (exp_first * SHARDS + shard_idx) * SLOT_CAP + slot_first, n_rows)
    row_two = jnp.where(slot_second >= 0, (exp_second * SHARDS + shard_idx) * SLOT_CAP + slot_second, n_rows)
    dy_float = tok_dy.astype(jnp.float32)
    grad_one = (gate_one[:, None] * dy_float).astype(jnp.bfloat16)
    grad_two = (gate_two[:, None] * dy_float).astype(jnp.bfloat16)
    empty_rows = jnp.zeros((n_rows, D_MODEL), jnp.bfloat16)
    hid_buf = empty_rows.at[row_one].set(hidden, mode='drop').at[row_two].set(hidden, mode='drop')
    grad_buf = empty_rows.at[row_one].set(grad_one, mode='drop').at[row_two].set(grad_two, mode='drop')
    exp_out, grad_hid, dw_gate, dw_up, dw_down = lax.map(
        expert_pass,
        (hid_buf.reshape(EXPERTS, SHARDS * SLOT_CAP, D_MODEL), grad_buf.reshape(EXPERTS, SHARDS * SLOT_CAP, D_MODEL),
         w_gate, w_up, w_down))
    exp_out = exp_out.reshape(n_rows, D_MODEL)
    grad_hid = grad_hid.reshape(n_rows, D_MODEL)
    out_one = jnp.take(exp_out, row_one, axis=0, mode='fill', fill_value=0).astype(jnp.float32)
    out_two = jnp.take(exp_out, row_two, axis=0, mode='fill', fill_value=0).astype(jnp.float32)
    y_mix = gate_one[:, None] * out_one + gate_two[:, None] * out_two
    out_tok = (tok_x.astype(jnp.float32) + y_mix).astype(jnp.bfloat16)
    dgate_one = jnp.sum(dy_float * out_one, axis=-1)
    dgate_two = jnp.sum(dy_float * out_two, axis=-1)
    d_logits = ((dgate_one * gate_one)[:, None] * (pick_one - prob_one)
                + (dgate_two * gate_two)[:, None] * (pick_two - prob_two)).astype(jnp.bfloat16)
    d_router = jnp.dot(hidden.T, d_logits, preferred_element_type=jnp.float32)
    grad_h = (jnp.dot(d_logits, router.T, preferred_element_type=jnp.float32)
              + jnp.take(grad_hid, row_one, axis=0, mode='fill', fill_value=0).astype(jnp.float32)
              + jnp.take(grad_hid, row_two, axis=0, mode='fill', fill_value=0).astype(jnp.float32))
    d_ln_weight = jnp.sum(grad_h * x_hat, axis=0)
    d_ln_bias = jnp.sum(grad_h, axis=0)
    dx_tok = (dy_float + layer_norm_back(grad_h, x_hat, inv_std, ln_weight)).astype(jnp.bfloat16)
    return (out_tok, dx_tok, dw_gate, dw_up, dw_down, d_router, d_ln_weight, d_ln_bias)
```

```python
import functools

import jax
import jax.numpy as jnp
from jax import lax
from jax.experimental import pallas as pl
from jax.experimental.pallas import tpu as pltpu
from jax.sharding import PartitionSpec as P

LN_EPS = 1e-5
N_CHUNK = 3
FF_BLOCK = 352
COL_BLOCK = 512
OUT_BLOCK = 256
SRC_BLOCK = 4
VMEM_BYTES = 60 * 1024 * 1024
f32 = jnp.float32
bf16 = jnp.bfloat16


def layer_norm(x_rows, ln_weight, ln_bias):
    x_float = x_rows.astype(jnp.float32)
    centered = x_float - jnp.mean(x_float, axis=-1, keepdims=True)
    inv_std = lax.rsqrt(jnp.mean(centered * centered, axis=-1, keepdims=True) + LN_EPS)
    x_hat = centered * inv_std
    hidden = (x_hat * ln_weight.astype(jnp.float32) + ln_bias.astype(jnp.float32)).astype(jnp.bfloat16)
    return hidden, x_hat, inv_std


def layer_norm_back(grad_h, x_hat, inv_std, ln_weight):
    scaled = grad_h * ln_weight.astype(jnp.float32)
    return inv_std * (scaled - jnp.mean(scaled, axis=-1, keepdims=True)
                      - x_hat * jnp.mean(scaled * x_hat, axis=-1, keepdims=True))


def masked_gate(logits, allowed, choice):
    expert_ids = jnp.arange(logits.shape[-1])
    prob_all = jax.nn.softmax(jnp.where(allowed, logits, -1e30), axis=-1)
    picked = (choice[:, None] == expert_ids[None, :]).astype(jnp.float32)
    return jnp.sum(prob_all * picked, axis=-1), prob_all, picked


def dot(lhs, rhs, lhs_dim, rhs_dim):
    return lax.dot_general(lhs, rhs, (((lhs_dim,), (rhs_dim,)), ((), ())), preferred_element_type=f32)


def once(shape, index):
    return pl.BlockSpec(shape, index, pipeline_mode=pl.Buffered(1))


def cost(flops, moved):
    return pl.CostEstimate(flops=flops, bytes_accessed=moved, transcendentals=0)


def mid_kernel(plane_ref, hid_ref, grad_ref, gate_ref, up_ref, down_ref, *refs):
    act_ref, back_gate_ref, back_up_ref = refs[-3:]
    rows = hid_ref.shape[-2]

    def block(i, carry):
        cols = pl.ds(pl.multiple_of(i * COL_BLOCK, COL_BLOCK), COL_BLOCK)
        hid = hid_ref[0, cols, :]
        pre_gate = dot(gate_ref[...], hid, 1, 1)
        pre_up = dot(up_ref[...], hid, 1, 1)
        grad_inner = dot(down_ref[...], grad_ref[0, cols, :], 1, 1)
        sig_gate = jax.nn.sigmoid(pre_gate)
        silu_gate = pre_gate * sig_gate
        act_ref[0, :, cols] = (silu_gate * pre_up).astype(bf16)
        back_gate_ref[0, :, cols] = (grad_inner * pre_up * sig_gate * (1.0 + pre_gate * (1.0 - sig_gate))).astype(bf16)
        back_up_ref[0, :, cols] = (grad_inner * silu_gate).astype(bf16)
        return carry

    lax.fori_loop(0, rows // COL_BLOCK, block, 0)


def expert_mid(source, target, hid, grad, weights, earlier=()):
    rows, d_model = hid.shape[1:]
    ff = weights[0].shape[0]
    planes = jnp.stack([source, target]).astype(jnp.int32)
    row_spec = once((1, rows, d_model), lambda j, p: (p[0], 0, 0))
    weight_spec = pl.BlockSpec((FF_BLOCK, d_model), lambda j, p: (j, 0))
    out_spec = pl.BlockSpec((1, FF_BLOCK, rows), lambda j, p: (p[1], j, 0))
    shape = jax.ShapeDtypeStruct((2, ff, rows), bf16)
    return pl.pallas_call(
        mid_kernel,
        grid_spec=pltpu.PrefetchScalarGridSpec(
            num_scalar_prefetch=1, grid=(pl.cdiv(ff, FF_BLOCK),),
            in_specs=[row_spec] * 2 + [weight_spec] * 3 + [pl.BlockSpec(memory_space=pl.ANY)] * len(earlier),
            out_specs=[out_spec] * 3),
        out_shape=[shape] * 3,
        input_output_aliases={6 + k: k for k in range(len(earlier))},
        cost_estimate=cost(6 * rows * ff * d_model, 4 * rows * d_model + 6 * ff * (d_model + rows)),
        compiler_params=pltpu.CompilerParams(vmem_limit_bytes=VMEM_BYTES),
        name="expert_mid")(planes, hid, grad, *weights, *earlier)


def back_kernel(count, plane_ref, *refs):
    lhs_refs, weight_refs, out_ref, turned = refs[:count], refs[count:2 * count], refs[-1 - count], refs[-count:]
    d_model = out_ref.shape[-1]
    for lhs_ref, turned_ref in zip(lhs_refs, turned):
        turned_ref[...] = lhs_ref[0].T

    def block(i, carry):
        cols = pl.ds(pl.multiple_of(i * COL_BLOCK, COL_BLOCK), COL_BLOCK)
        total = dot(turned[0][...], weight_refs[0][:, cols], 1, 0)
        for turned_ref, weight_ref in zip(turned[1:], weight_refs[1:]):
            total = total + dot(turned_ref[...], weight_ref[:, cols], 1, 0)
        out_ref[:, :, cols] = total.astype(bf16).reshape(out_ref.shape[:2] + (COL_BLOCK,))
        return carry

    lax.fori_loop(0, d_model // COL_BLOCK, block, 0)


def expert_back(plane, lhs, weights, chunk, n_src, slot_cap, earlier=()):
    ff, d_model = weights[0].shape
    rows = lhs[0].shape[2]
    part = rows // n_src
    count = len(lhs)
    block = SRC_BLOCK * part
    return pl.pallas_call(
        functools.partial(back_kernel, count),
        grid_spec=pltpu.PrefetchScalarGridSpec(
            num_scalar_prefetch=1, grid=(n_src // SRC_BLOCK,),
            in_specs=[pl.BlockSpec((1, ff, block), lambda j, p: (p[0], 0, j))] * count
            + [once((ff, d_model), lambda j, p: (0, 0))] * count + [pl.BlockSpec(memory_space=pl.ANY)] * len(earlier),
            out_specs=pl.BlockSpec((SRC_BLOCK, part, d_model), lambda j, p: (j, chunk, 0)),
            scratch_shapes=[pltpu.VMEM((block, ff), bf16)] * count),
        out_shape=jax.ShapeDtypeStruct((n_src, slot_cap, d_model), bf16),
        input_output_aliases={1 + 2 * count + k: k for k in range(len(earlier))},
        cost_estimate=cost(2 * count * rows * ff * d_model, 2 * (count * ff * (d_model + rows) + rows * d_model)),
        compiler_params=pltpu.CompilerParams(vmem_limit_bytes=VMEM_BYTES),
        name="expert_back")(plane.reshape(1).astype(jnp.int32), *lhs, *weights, *earlier)


def grads_kernel(act_ref, back_gate_ref, back_up_ref, hid_ref, grad_ref, *refs):
    ff = act_ref.shape[1]
    half = ff // 2

    def block(i, carry):
        rows = pl.ds(pl.multiple_of(i * half, 16), half)
        for k, (lhs_ref, rhs_ref) in enumerate(((back_gate_ref, hid_ref), (back_up_ref, hid_ref), (act_ref, grad_ref))):
            total = dot(lhs_ref[0, rows, :], rhs_ref[0], 1, 0) + dot(lhs_ref[1, rows, :], rhs_ref[1], 1, 0)
            if len(refs) > 3:
                total = total + refs[k][rows, :]
            refs[-3 + k][rows, :] = total
        return carry

    lax.fori_loop(0, 2, block, 0)


def expert_grads(act, back_gate, back_up, hid_all, grad_all, earlier=()):
    planes, rows, d_model = hid_all.shape
    ff = act.shape[1]
    lhs_spec = once((planes, ff, rows), lambda j: (0, 0, 0))
    rhs_spec = pl.BlockSpec((planes, rows, OUT_BLOCK), lambda j: (0, 0, j))
    out_spec = pl.BlockSpec((ff, OUT_BLOCK), lambda j: (0, j))
    return pl.pallas_call(
        grads_kernel,
        grid=(d_model // OUT_BLOCK,),
        in_specs=[lhs_spec] * 3 + [rhs_spec] * 2 + [out_spec] * len(earlier),
        out_specs=[out_spec] * 3,
        out_shape=[jax.ShapeDtypeStruct((ff, d_model), f32)] * 3,
        input_output_aliases={5 + k: k for k in range(len(earlier))},
        cost_estimate=cost(12 * rows * ff * d_model, 12 * ff * (rows + 2 * d_model) + 8 * rows * d_model),
        compiler_params=pltpu.CompilerParams(vmem_limit_bytes=VMEM_BYTES),
        name="expert_grads")(act, back_gate, back_up, hid_all, grad_all, *earlier)


def solution(mesh):
    n_ep = mesh.shape['ep']
    tok_spec = P(('dp', 'ep'), None)
    row_spec = P(('dp', 'ep'))
    exp_spec = P('ep', None, None)

    def local_step(tok_x, tok_dy, exp_first, exp_second, eligible, slot_first, slot_second,
                   ln_weight, ln_bias, router, w_gate, w_up, w_down):
        n_local, d_model = tok_x.shape
        n_exp = eligible.shape[1]
        weights = (w_gate[0].T, w_up[0].T, w_down[0])
        slot_cap = 3 * n_local // n_exp
        part = slot_cap // N_CHUNK
        dp_index = lax.axis_index('dp')
        hidden, x_hat, inv_std = layer_norm(tok_x, ln_weight, ln_bias)
        logits = jnp.dot(hidden, router, preferred_element_type=f32)
        expert_ids = jnp.arange(n_exp)
        allowed = eligible > 0
        gate_one, prob_one, pick_one = masked_gate(logits, allowed, exp_first)
        gate_two, prob_two, pick_two = masked_gate(logits, allowed & (expert_ids[None, :] != exp_first[:, None]), exp_second)

        def select(choice, slot, start, part):
            rel = slot - start
            pos = jnp.where((rel >= 0) & (rel < part), choice * part + rel, -1)
            return pos[:, None] == jnp.arange(n_exp * part)[None, :]

        def exchange(buf, part):
            return lax.all_to_all(buf.reshape(n_ep, part, d_model), 'ep', 0, 0, tiled=True)

        last = []

        def chain(*arrays):
            tied = lax.optimization_barrier(tuple(arrays) + tuple(last))
            return tied[:len(arrays)]

        def done(*arrays):
            last[:] = arrays

        dy_float = tok_dy.astype(f32)
        hid_buf, grad_buf = [], []
        for c in range(N_CHUNK):
            one, two = select(exp_first, slot_first, c * part, part), select(exp_second, slot_second, c * part, part)
            sel_both = one.astype(bf16) + two.astype(bf16)
            gate_row = jnp.sum(jnp.where(one, gate_one[:, None], 0.0) + jnp.where(two, gate_two[:, None], 0.0), axis=0)
            hid_in, = chain(hidden)
            hid_buf.append(dot(sel_both, hid_in, 0, 0).astype(bf16))
            done(hid_buf[-1])
            dy_in, = chain(tok_dy)
            grad_buf.append((dot(sel_both, dy_in, 0, 0) * gate_row[:, None]).astype(bf16))
            done(grad_buf[-1])
        hid_recv, grad_recv, hid_all, grad_all = [], [], [], []
        previous = []
        for c in range(N_CHUNK):
            for buf, recv, both in ((hid_buf[c], hid_recv, hid_all), (grad_buf[c], grad_recv, grad_all)):
                buf = lax.optimization_barrier((buf, *previous))[0]
                recv.append(exchange(buf, part).reshape(n_exp * part, d_model))
                previous = [recv[-1]]
                both.append(lax.all_gather(recv[-1], 'dp'))

        middle = [None] * N_CHUNK
        exp_out, grad_hid, weight_grads = (), (), ()

        def mid_own(c):
            rows, grads = chain(hid_recv[c][None], grad_recv[c][None])
            middle[c] = expert_mid(0 * dp_index, dp_index, rows, grads, weights)
            done(*middle[c])

        def mid_far(c):
            rows, grads = chain(hid_all[c], grad_all[c])
            middle[c] = expert_mid(1 - dp_index, 1 - dp_index, rows, grads, weights, middle[c])
            done(*middle[c])

        def rows_back(lhs, lhs_weights, c, earlier):
            lhs = chain(*lhs)
            out = expert_back(dp_index, lhs, lhs_weights, c, n_ep, slot_cap, earlier)
            done(out)
            return (out,)

        def weight_back(c, earlier):
            act, back_gate, back_up = chain(*middle[c])
            out = expert_grads(act, back_gate, back_up, hid_all[c], grad_all[c], earlier)
            done(*out)
            return out

        for c in range(N_CHUNK):
            if c == N_CHUNK - 1:
                mid_far(0)
            mid_own(c)
            exp_out = rows_back(middle[c][:1], weights[2:], c, exp_out)
            grad_hid = rows_back(middle[c][1:], weights[:2], c, grad_hid)
        out_back = exchange(lax.optimization_barrier((exp_out[0], *previous))[0], slot_cap).reshape(-1, d_model)
        hid_back = exchange(lax.optimization_barrier((grad_hid[0], out_back))[0], slot_cap).reshape(-1, d_model)
        weight_grads = weight_back(0, weight_grads)
        mid_far(1)
        weight_grads = weight_back(1, weight_grads)
        out_in, = chain(out_back)
        sel_one = select(exp_first, slot_first, 0, slot_cap).astype(bf16)
        sel_two = select(exp_second, slot_second, 0, slot_cap).astype(bf16)
        out_one = dot(sel_one, out_in, 1, 0)
        out_two = dot(sel_two, out_in, 1, 0)
        y_mix = gate_one[:, None] * out_one + gate_two[:, None] * out_two
        out_tok = (tok_x.astype(f32) + y_mix).astype(bf16)
        dgate_one = jnp.sum(dy_float * out_one, axis=-1)
        dgate_two = jnp.sum(dy_float * out_two, axis=-1)
        d_logits = ((dgate_one * gate_one)[:, None] * (pick_one - prob_one)
                    + (dgate_two * gate_two)[:, None] * (pick_two - prob_two)).astype(bf16)
        d_router = jnp.einsum('td,te->de', hidden, d_logits, preferred_element_type=f32)
        done(out_tok, d_router)
        hid_in, = chain(hid_back)
        grad_exp = dot(sel_one + sel_two, hid_in, 1, 0)
        grad_h = jnp.einsum('te,de->td', d_logits, router, preferred_element_type=f32) + grad_exp
        d_ln_weight = jnp.sum(grad_h * x_hat, axis=0)
        d_ln_bias = jnp.sum(grad_h, axis=0)
        dx_tok = (dy_float + layer_norm_back(grad_h, x_hat, inv_std, ln_weight)).astype(bf16)
        done(dx_tok)
        mid_far(2)
        dw_gate, dw_up, dw_down = weight_back(2, weight_grads)
        d_router = lax.psum(d_router, ('dp', 'ep'))
        d_ln_weight = lax.psum(d_ln_weight, ('dp', 'ep'))
        d_ln_bias = lax.psum(d_ln_bias, ('dp', 'ep'))
        return out_tok, dx_tok, dw_gate.T[None], dw_up.T[None], dw_down[None], d_router, d_ln_weight, d_ln_bias

    return jax.shard_map(
        local_step, mesh=mesh,
        in_specs=(tok_spec, tok_spec, row_spec, row_spec, tok_spec, row_spec, row_spec,
                  P(), P(), P(), exp_spec, exp_spec, exp_spec),
        out_specs=(tok_spec, tok_spec, exp_spec, exp_spec, exp_spec, P(), P(), P()),
        check_vma=False)
```
